32 devices in a mesh: fsdp: 8 (over z, x), rep: 4 (over y, core).
Axes of the slice: x: 2, y: 2, z: 4, core: 2. Of those that a mesh axis runs over, the one named last changes fastest.
Arguments:
- partials: bfloat16 [4, 56, 1024, 1024], P('rep', None, 'fsdp'), may hold values from -400 to 400
- sketch: bfloat16 [8, 4, 2, 1024, 256], P('fsdp', 'rep'), may hold values from -3 to 3
- owner_table: int32 [56, 1], replicated, may hold values from 0 to 7; in each aligned block of 14 rows (0 to 13, 14 to 27, ...) at most 2 rows name the same one
Outputs:
- update: bfloat16 [56, 1024, 1024], P('rep', 'fsdp')
- new_sketch: bfloat16 [8, 4, 2, 1024, 256], P('fsdp', 'rep')
The draws below stay inside these ranges and needn't reach their ends.
Inputs may be any that keep to these rules, and one draw needn't show every extreme that they name: `owner_table`: in each aligned slice of 14 blocks no owner holds more than 2 blocks; some owner holds exactly 2 in some slice.
All inputs are finite; a program needn't handle non-finite values.
Results may differ from the reference program's by a relative error of at most 0.015.
Values may be sent and summed in bfloat16 or wider, within the bound.
No kernel may reach another device: no remote copies, remote signals or barrier semaphores. Data moves between devices by JAX's collectives and lax.ppermute only.
A program may use at most 128 MiB of HBM per device.

```python
import math
import jax
import jax.numpy as jnp
import numpy as np
from jax import lax

BS = 1024
RANK = 256
SLOTS = 2
NS_ITERS = 5
BLK_REP = 14
NB = 56
N_FSDP = 8
N_REP = 4


def draw_partials(key, part):
    row_key, column_key, noise_key = jax.random.split(key, 3)
    row_scale = jnp.exp(jax.random.uniform(row_key, (NB, BS, 1), jnp.float32) * math.log(10.0))
    column_scale = jnp.exp(jax.random.uniform(column_key, (NB, 1, BS), jnp.float32) * math.log(10.0))
    block_place = jnp.arange(NB, dtype=jnp.float32) / NB
    row_place = jnp.arange(BS, dtype=jnp.float32) / BS
    trend = jnp.exp(0.5 * math.log(3.0) * (block_place[:, None, None] + row_place[None, :, None]))
    amplitude = 0.1 * row_scale * column_scale * trend

    def replica(number):
        noise = jnp.clip(jax.random.normal(jax.random.fold_in(noise_key, number), (NB, BS, BS), jnp.float32), -6.0, 6.0)
        return (amplitude * noise).astype(jnp.bfloat16)
    return lax.map(replica, jnp.arange(N_REP, dtype=jnp.int32))


def steps_of(stream_key, dims, shards, smallest, top_value):
    level, own = 1.0, jax.random.fold_in(stream_key, 6)
    for axis_at, shards_of in shards:
        steps = jnp.exp(jax.random.uniform(jax.random.fold_in(own, axis_at), (shards_of,), jnp.float32, smallest / len(shards), top_value / len(shards)))
        level = level * jnp.repeat(steps, dims[axis_at] // shards_of).reshape([-1 if axis == axis_at else 1 for axis in range(len(dims))])
    return level


def assign_block(own_key, own, number, rows, number_of, top, bound, slope):
    ranking = jax.random.permutation(own_key, number_of)
    heavy_load, ordinary = load_shares(number_of, rows * top, bound, slope, True), load_shares(number_of, rows * top, bound, slope, False)
    places = jnp.arange(number_of)

    def named(lengths, offset_by):
        used = int((lengths > 0).sum())
        fixed = max(1, used // 4)
        shifted = fixed + (places - fixed + offset_by * (used - fixed)) % max(1, number_of - fixed)
        return jnp.zeros((number_of,), jnp.int32).at[ranking[jnp.where(places < fixed, places, shifted)]].set(jnp.asarray(lengths, jnp.int32))

    lengths = jnp.where(number % 4 == 0, named(heavy_load, number // 4), named(ordinary, number - number // 4 - 1))
    mixed = jax.random.permutation(jax.random.fold_in(own, 3), number_of)
    giver, taker = mixed[0:number_of // 2 * 2:2], mixed[1:number_of // 2 * 2:2]
    slack = jnp.minimum(lengths[giver] - 1, bound - lengths[taker]) // 2
    slack = jnp.where((giver == ranking[0]) | (taker == ranking[0]) | (lengths[taker] == 0), 0, jnp.maximum(slack, 0))
    shifted = jax.random.randint(jax.random.fold_in(own, 4), (number_of // 2,), 0, 1 << 20) % (slack + 1)
    lengths = lengths.at[giver].add(-shifted).at[taker].add(shifted)
    labels = jnp.searchsorted(jnp.cumsum(lengths), jnp.arange(rows * top), side="right").astype(jnp.int32)
    grid = labels.reshape(top, rows).T
    grid = grid[jax.random.permutation(jax.random.fold_in(own, 1), rows)]
    offset_by = jax.random.randint(jax.random.fold_in(own, 2), (rows, 1), 0, top)
    return jnp.take_along_axis(grid, (jnp.arange(top)[None, :] + offset_by) % top, axis=1)


def load_shares(amount, total, reach, slope, full):
    portions = [(1 << 20) // math.isqrt(standing ** slope) + 1 for standing in range(1, amount + 1)]
    largest = reach if full else min(reach, max(-(-total // amount), total * portions[0] // sum(portions)))
    least = 1 if total - largest >= amount - 1 else 0
    holding, rest = [largest] + [least] * (amount - 1), total - largest - least * (amount - 1)
    while rest > 0:
        movable = [i for i in range(1, amount) if holding[i] < largest] or [i for i in range(1, amount) if holding[i] < reach]
        mass, remaining = sum([portions[i] for i in movable]), rest
        for i in movable:
            extra = min(reach - holding[i], max(1, remaining * portions[i] // mass), rest)
            holding[i] = holding[i] + extra
            rest = rest - extra
    return np.array(holding)


def bell_draw(own_key, shape, scale, most, cuts=(), kind=jnp.bfloat16):
    factor_of = steps_of(own_key, shape, cuts, -0.22, 0.18) if cuts else 1.0
    array = jax.random.normal(own_key, shape, jnp.float32) * scale * factor_of
    return jnp.minimum(jnp.maximum(array, -most), most).astype(kind)


def setup_inputs(seed: int = 0) -> dict:
    seeds = jax.random.split(jax.random.key(seed), 4)
    partials = draw_partials(jax.random.fold_in(seeds[3], 71), 0)
    sketch = bell_draw(seeds[1], (N_FSDP, N_REP, SLOTS, BS, RANK), 0.5, 3.0, ((0, 8), (1, 4)))
    owner_table_keys = jax.random.split(jax.random.fold_in(seeds[2], 1), NB // BLK_REP)
    owner_table_turns = jax.random.permutation(jax.random.fold_in(seeds[2], 3), NB // BLK_REP)
    owner_table = jax.vmap(lambda own, number: assign_block(jax.random.fold_in(seeds[2], 2), own, number, BLK_REP, N_FSDP, 1, SLOTS, 2))(owner_table_keys, owner_table_turns).reshape((NB, 1))
    return {"partials": partials, "sketch": sketch, "owner_table": owner_table}


DECAY = 0.9
DAMPING = 64.0
FIRST_AXES = (((0,), (0,)), ((), ()))
LAST_AXES = (((1,), (1,)), ((), ()))

def inverse_root(matrix, epsilon):
    identity = jnp.eye(matrix.shape[0], dtype=jnp.float32)
    trace_sum = jnp.trace(matrix) + epsilon
    current = matrix / trace_sum
    inverse = identity
    for repeat in range(NS_ITERS):
        middle = 1.5 * identity - 0.5 * jnp.dot(inverse, current, precision=lax.Precision.HIGHEST)
        current = jnp.dot(current, middle, precision=lax.Precision.HIGHEST)
        inverse = jnp.dot(middle, inverse, precision=lax.Precision.HIGHEST)
    return inverse / jnp.sqrt(trace_sum)

def precondition(gradient, current_sketch):
    identity = jnp.eye(current_sketch.shape[1], dtype=jnp.float32)
    projected = lax.dot_general(gradient, current_sketch, FIRST_AXES, preferred_element_type=jnp.float32).astype(jnp.bfloat16)
    gram_matrix = lax.dot_general(current_sketch, current_sketch, FIRST_AXES, preferred_element_type=jnp.float32).astype(jnp.bfloat16)
    powered = DECAY * jnp.dot(current_sketch, gram_matrix, preferred_element_type=jnp.float32) + jnp.dot(gradient, projected, preferred_element_type=jnp.float32)
    inner_gram = lax.dot_general(powered, powered, FIRST_AXES, precision=lax.Precision.HIGHEST)
    basis_full = jnp.dot(powered, inverse_root(inner_gram, 1e-06), precision=lax.Precision.HIGHEST)
    basis_low = basis_full.astype(jnp.bfloat16)
    coefficients = lax.dot_general(gradient, basis_low, FIRST_AXES, preferred_element_type=jnp.float32).astype(jnp.bfloat16)
    alignment = lax.dot_general(current_sketch, basis_low, FIRST_AXES, preferred_element_type=jnp.float32)
    energy = DECAY * lax.dot_general(alignment, alignment, FIRST_AXES, precision=lax.Precision.HIGHEST) + lax.dot_general(coefficients, coefficients, FIRST_AXES, preferred_element_type=jnp.float32)
    root_inverse = inverse_root(energy + DAMPING * identity, 0.0)
    inner_part = jnp.dot(energy, root_inverse, precision=lax.Precision.HIGHEST)
    new_block = jnp.dot(basis_full, inner_part, precision=lax.Precision.HIGHEST).astype(jnp.bfloat16)
    mix_matrix = math.sqrt(DAMPING) * root_inverse - identity
    side_terms = lax.dot_general(coefficients.astype(jnp.float32), mix_matrix, LAST_AXES, precision=lax.Precision.HIGHEST).astype(jnp.bfloat16)
    update_block = (gradient.astype(jnp.float32) + lax.dot_general(basis_low, side_terms, LAST_AXES, preferred_element_type=jnp.float32)).astype(jnp.bfloat16)
    return (update_block, new_block)

def reference(partials, sketch, owner_table):
    owner_ids = owner_table[:, 0]
    block_ids = jnp.arange(NB, dtype=jnp.int32)

    def reduce_block(block):
        replicas = lax.dynamic_index_in_dim(partials, block, axis=1, keepdims=False)
        summed = lax.optimization_barrier(jnp.sum(replicas.astype(jnp.float32), axis=0)).astype(jnp.bfloat16)
        wide = summed.astype(jnp.float32)
        return (summed, jnp.sum(wide * wide))
    gradients, squares = lax.map(reduce_block, block_ids)
    sum_squares = jnp.sum(squares)
    clip_limit = 0.5 * math.sqrt(NB * BS * BS)
    clip_factor = jnp.minimum(1.0, clip_limit / jnp.sqrt(sum_squares + 1e-06))
    slice_ids = block_ids // BLK_REP
    same_owner = (owner_ids[:, None] == owner_ids[None, :]) & (slice_ids[:, None] == slice_ids[None, :]) & (block_ids[:, None] < block_ids[None, :])
    rank_in = lax.optimization_barrier(jnp.sum(same_owner.astype(jnp.int32), axis=0))

    def per_block(block):
        gradient = (clip_factor * gradients[block].astype(jnp.float32)).astype(jnp.bfloat16)
        current_sketch = sketch[owner_ids[block], slice_ids[block], rank_in[block]]
        return precondition(gradient, current_sketch)
    update, fresh_blocks = lax.map(per_block, block_ids)
    new_sketch = sketch.at[owner_ids, slice_ids, rank_in].set(fresh_blocks)
    return (update, new_sketch)
```

```python
import math

import jax
import jax.numpy as jnp
from jax import lax
from jax.experimental import pallas as pl
from jax.experimental.pallas import tpu as pltpu
from jax.sharding import PartitionSpec as P


NS_ITERS = 5
DECAY = 0.9
DAMPING = 64.0
CORES = 2
PARTS = 2
NN = (((1,), (0,)), ((), ()))
NT = (((1,), (1,)), ((), ()))


def dot(left, right, dims=NN):
    return lax.dot_general(left, right, dims, preferred_element_type=jnp.float32)


def split(value):
    high = value.astype(jnp.bfloat16)
    return high, (value - high.astype(jnp.float32)).astype(jnp.bfloat16)


def dot3(left, right, dims=NN):
    return dot(left[0], right[0], dims) + (
        dot(left[0], right[1], dims) + dot(left[1], right[0], dims)
    )


def diagonal(size):
    rows = lax.broadcasted_iota(jnp.int32, (size, size), 0)
    return rows == lax.broadcasted_iota(jnp.int32, (size, size), 1)


def inverse_root(matrix, epsilon):
    on_diagonal = diagonal(matrix.shape[0])
    trace_sum = jnp.sum(jnp.where(on_diagonal, matrix, 0.0), axis=(0, 1), keepdims=True) + epsilon
    current = matrix / trace_sum
    three_halves = jnp.where(on_diagonal, 1.5, 0.0)
    middle = three_halves - 0.5 * current
    inverse = middle
    middle_pair = split(middle)
    current_pair = split(current)
    for _ in range(1, NS_ITERS):
        current_pair = split(dot3(current_pair, middle_pair))
        inverse_pair = split(inverse)
        middle = three_halves - 0.5 * dot3(inverse_pair, current_pair)
        middle_pair = split(middle)
        inverse = dot3(middle_pair, inverse_pair)
    return inverse * lax.rsqrt(trace_sum)


def precondition_kernel(slot_ref, clip_ref, sketch_ref, *rest):
    *arrived_refs, update_ref, new_ref, gradient_ref = rest
    clip = clip_ref[0, 0]
    for number, piece_ref in enumerate(arrived_refs):
        across = piece_ref.shape[1]
        gradient_ref[:, number * across : (number + 1) * across] = (
            piece_ref[...].astype(jnp.float32) * clip
        ).astype(jnp.bfloat16)
    held = sketch_ref[slot_ref[0]]
    rank = held.shape[1]
    held_t = held.T
    projected_t = dot(held_t, gradient_ref[...]).astype(jnp.bfloat16)
    gram = dot(held_t, held).astype(jnp.bfloat16)
    powered_t = DECAY * dot(gram, held_t) + dot(projected_t, gradient_ref[...], NT)
    powered_pair = split(powered_t)
    root = inverse_root(dot3(powered_pair, powered_pair, NT), 1e-06)
    basis_t = dot3(split(root), powered_pair)
    basis_pair = split(basis_t)
    basis_low_t = basis_pair[0]
    coefficients_t = dot(basis_low_t, gradient_ref[...]).astype(jnp.bfloat16)
    alignment_pair = split(dot(basis_low_t, held))
    energy = DECAY * dot3(alignment_pair, alignment_pair, NT) + dot(
        coefficients_t, coefficients_t, NT
    )
    on_diagonal = diagonal(rank)
    root_inverse = inverse_root(energy + jnp.where(on_diagonal, DAMPING, 0.0), 0.0)
    mix = math.sqrt(DAMPING) * root_inverse - jnp.where(on_diagonal, 1.0, 0.0)
    mix_pair = split(mix)
    side_t = (dot(mix_pair[0], coefficients_t) + dot(mix_pair[1], coefficients_t)).astype(
        jnp.bfloat16
    )
    update_ref[...] = (
        gradient_ref[...].astype(jnp.float32) + dot(basis_low_t.T, side_t)
    ).astype(jnp.bfloat16)
    inner = dot3(split(root_inverse), split(energy))
    new_ref[...] = dot3(split(inner), basis_pair).astype(jnp.bfloat16).T


def precondition(slot, clip, arrived, held):
    width, rank = held.shape[1:]
    return pl.pallas_call(
        precondition_kernel,
        out_shape=(
            jax.ShapeDtypeStruct((width, width), jnp.bfloat16),
            jax.ShapeDtypeStruct((width, rank), jnp.bfloat16),
        ),
        in_specs=[
            pl.BlockSpec(memory_space=pltpu.SMEM),
            pl.BlockSpec(memory_space=pltpu.SMEM),
            *[pl.BlockSpec(memory_space=pltpu.VMEM)] * (1 + len(arrived)),
        ],
        out_specs=(
            pl.BlockSpec(memory_space=pltpu.VMEM),
            pl.BlockSpec(memory_space=pltpu.VMEM),
        ),
        scratch_shapes=[pltpu.VMEM((width, width), jnp.bfloat16)],
        compiler_params=pltpu.CompilerParams(vmem_limit_bytes=48 * 2**20),
        cost_estimate=pl.CostEstimate(
            flops=24 * width * width * rank, bytes_accessed=6 * width * width, transcendentals=0
        ),
        name="precondition",
    )(slot, clip, held, *arrived)


class Piece:
    def __init__(self, start, count, part, parts, per_slice, partial, source):
        self.start, self.count, self.per_slice = start, count, per_slice
        self.partial, self.source = partial, source
        self.rows, self.width = partial.shape[1], partial.shape[2] // parts
        self.first_column = part * self.width
        self.shape = jax.ShapeDtypeStruct((count, self.rows, self.width), partial.dtype)

    def copies(self, which, source_ref, slices_ref, partial_ref, held_ref, semaphores):
        base = slices_ref[which] * self.per_slice + self.start
        columns = pl.ds(self.first_column, self.width)
        return [
            pltpu.make_async_copy(
                partial_ref.at[source_ref[base + at], :, columns], held_ref.at[at], semaphores.at[at]
            )
            for at in range(self.count)
        ]

    def call(self, kernel, slices, operands, out_shape, scalars=()):
        return pl.pallas_call(
            kernel,
            out_shape=out_shape,
            in_specs=[pl.BlockSpec(memory_space=pltpu.SMEM)] * (2 + len(scalars))
            + [pl.BlockSpec(memory_space=pl.ANY)]
            + [pl.BlockSpec(memory_space=pltpu.VMEM)] * len(operands),
            out_specs=jax.tree.map(lambda _: pl.BlockSpec(memory_space=pltpu.VMEM), out_shape),
            scratch_shapes=[
                pltpu.VMEM(self.shape.shape, self.shape.dtype),
                pltpu.SemaphoreType.DMA((self.count,)),
            ],
        )(self.source, slices, *scalars, self.partial, *operands)

    def add(self, which, slices, other):
        def kernel(source_ref, slices_ref, partial_ref, other_ref, out_ref, held_ref, semaphores):
            copies = self.copies(which, source_ref, slices_ref, partial_ref, held_ref, semaphores)
            for copy in copies:
                copy.start()
            for at, copy in enumerate(copies):
                copy.wait()
                total = held_ref[at].astype(jnp.float32) + other_ref[at].astype(jnp.float32)
                out_ref[at] = total.astype(out_ref.dtype)

        return self.call(kernel, slices, [other], self.shape)

    def total(self, which, slices, others, index, valid):
        owners = index.shape[0]

        def kernel(source_ref, slices_ref, index_ref, valid_ref, partial_ref, *rest):
            *other_refs, out_ref, square_ref, held_ref, semaphores = rest
            copies = self.copies(which, source_ref, slices_ref, partial_ref, held_ref, semaphores)
            for copy in copies:
                copy.start()
            for copy in copies:
                copy.wait()
            square_ref[...] = jnp.zeros_like(square_ref)

            @pl.loop(0, owners)
            def _(owner):
                at = index_ref[owner]
                total = held_ref[at].astype(jnp.float32)
                for other_ref in other_refs:
                    total = total + other_ref[at].astype(jnp.float32)
                rounded = total.astype(out_ref.dtype)
                out_ref[owner] = rounded
                wide = rounded.astype(jnp.float32)
                squares = jnp.sum((wide * wide).reshape(-1, 8, wide.shape[-1]), axis=0)
                square_ref[...] += jnp.where(valid_ref[owner] > 0, squares, 0.0)

        out_shape = (
            jax.ShapeDtypeStruct((owners, self.rows, self.width), self.partial.dtype),
            jax.ShapeDtypeStruct((8, self.width), jnp.float32),
        )
        return self.call(kernel, slices, others, out_shape, (index, valid))


def pick_blocks(pieces, which, slices):
    counts = [piece.count for piece in pieces]

    def kernel(source_ref, slices_ref, partial_ref, *rest):
        *out_refs, semaphores = rest
        copies = [
            copy
            for number, (piece, out_ref) in enumerate(zip(pieces, out_refs))
            for copy in piece.copies(
                which, source_ref, slices_ref, partial_ref, out_ref, semaphores.at[number]
            )
        ]
        for copy in copies:
            copy.start()
        for copy in copies:
            copy.wait()

    return pl.pallas_call(
        kernel,
        out_shape=[piece.shape for piece in pieces],
        in_specs=[pl.BlockSpec(memory_space=pltpu.SMEM)] * 2 + [pl.BlockSpec(memory_space=pl.ANY)],
        out_specs=[pl.BlockSpec(memory_space=pltpu.VMEM) for _ in pieces],
        scratch_shapes=[pltpu.SemaphoreType.DMA((len(pieces), max(counts)))],
        name="pick_blocks",
    )(pieces[0].source, slices, pieces[0].partial)


def place_kernel(source_index_ref, target_index_ref, source_ref, *rest):
    out_ref, semaphores = rest[-2:]
    copies = [
        pltpu.make_async_copy(
            source_ref.at[source_index_ref[at]], out_ref.at[target_index_ref[at]], semaphores.at[at]
        )
        for at in range(semaphores.shape[0])
    ]
    for copy in copies:
        copy.start()
    for copy in copies:
        copy.wait()


def place_blocks(source_index, target_index, source, total, onto=None):
    smem = pl.BlockSpec(memory_space=pltpu.SMEM)
    anywhere = pl.BlockSpec(memory_space=pl.ANY)
    onto_list = [] if onto is None else [onto]
    return pl.pallas_call(
        place_kernel,
        in_specs=[smem, smem, pl.BlockSpec(memory_space=pltpu.VMEM)] + [anywhere] * len(onto_list),
        out_specs=anywhere,
        out_shape=jax.ShapeDtypeStruct((total,) + source.shape[1:], source.dtype),
        scratch_shapes=[pltpu.SemaphoreType.DMA(source_index.shape)],
        input_output_aliases={3: 0} if onto_list else {},
        name="place_blocks",
    )(source_index, target_index, source, *onto_list)


def total_over(value, axis):
    size = lax.axis_size(axis)
    if size & (size - 1):
        return lax.psum(value, axis)
    spread = jnp.full((8, 128), value)
    apart = 1
    while apart < size:
        spread = spread + lax.ppermute(spread, axis, [(at, at ^ apart) for at in range(size)])
        apart *= 2
    return spread[0, 0]


def local(partials, sketch, owner_table):
    block_total, row_count, block_width = partials.shape[1:]
    fsdp_count = lax.axis_size("fsdp")
    rep_count = lax.axis_size("rep")
    per_slice = block_total // rep_count
    held_sketches = sketch[0, 0]
    half_sizes = ((per_slice + 1) // 2, per_slice // 2)
    half_starts = (0, half_sizes[0])

    owners = owner_table[:, 0].reshape(rep_count, per_slice)
    places = jnp.arange(per_slice, dtype=jnp.int32)
    before = (places[:, None] < places[None, :])[None]
    same = owners[:, :, None] == owners[:, None, :]
    alone = jnp.sum(same.astype(jnp.int32), axis=1) == 1
    rank_in = jnp.sum((same & before).astype(jnp.int32), axis=1)
    alone_rank = jnp.sum((alone[:, :, None] & before).astype(jnp.int32), axis=1)
    alone_count = jnp.sum(alone.astype(jnp.int32), axis=1, keepdims=True)
    half = jnp.where(alone, (2 * alone_rank >= alone_count).astype(jnp.int32), rank_in)
    in_half = jnp.sum(((half[:, :, None] == half[:, None, :]) & before).astype(jnp.int32), axis=1)
    target = half * half_sizes[0] + in_half
    order = jnp.sum(
        jnp.where(target[:, :, None] == places[None, None, :], places[None, :, None], 0), axis=1
    )
    source = order + per_slice * jnp.arange(rep_count, dtype=jnp.int32)[:, None]

    my_slice = lax.axis_index("rep")
    my_owners, my_half, my_in_half, my_order = (
        lax.dynamic_index_in_dim(value, my_slice, 0, keepdims=False)
        for value in (owners, half, in_half, order)
    )
    owner_ids = jnp.arange(fsdp_count, dtype=jnp.int32)
    mine = my_owners == lax.axis_index("fsdp")
    both = jnp.sum(mine.astype(jnp.int32)) > 1

    partial = partials[0]
    outer_count = rep_count // CORES
    my_outer, my_core = my_slice // CORES, my_slice % CORES
    outers = (my_outer + jnp.arange(outer_count, dtype=jnp.int32)) % outer_count
    slices = jnp.concatenate([outers * CORES + (CORES - 1 - my_core), outers * CORES + my_core])
    source = source.reshape(-1)
    swap = [(at, at ^ 1) for at in range(rep_count)]

    pieces = [
        Piece(half_starts[number], half_sizes[number], part, PARTS, per_slice, partial, source)
        for number in range(2)
        for part in range(PARTS)
    ]
    others = [[] for _ in pieces]
    for step in range(1, outer_count):
        onward = [(at, (at + step * CORES) % rep_count) for at in range(rep_count)]
        picked = pick_blocks(pieces[:1], step, slices)
        later_slices, picked = lax.optimization_barrier((slices, picked))
        picked = picked + pick_blocks(pieces[1:], step, later_slices)
        for piece, sent, gathered in zip(pieces, picked, others):
            crossed = lax.ppermute(sent, "rep", swap)
            summed = piece.add(outer_count + step, later_slices, crossed)
            gathered.append(lax.ppermute(summed, "rep", onward))
            later_slices, _ = lax.optimization_barrier((later_slices, summed))
        slices = later_slices
    own = pick_blocks(pieces, 0, slices)
    for gathered, sent in zip(others, own):
        gathered.append(lax.ppermute(sent, "rep", swap))

    arrived, sums, clip_factor = [], [], None
    for number, (piece, gathered) in enumerate(zip(pieces, others)):
        holds = (my_owners[:, None] == owner_ids[None, :]) & (my_half[:, None] == number // PARTS)
        index = jnp.sum(jnp.where(holds, my_in_half[:, None], 0), axis=0)
        valid = jnp.sum(holds.astype(jnp.int32), axis=0)
        if number >= 2:
            gathered[0], arrived[number - 2] = lax.optimization_barrier(
                (gathered[0], arrived[number - 2])
            )
        laid_out, square = piece.total(outer_count, slices, gathered, index, valid)
        sums.append(jnp.sum(square))
        if number == len(pieces) - 1:
            sum_squares = total_over(total_over(sum(sums), "rep"), "fsdp")
            clip_limit = 0.5 * math.sqrt(block_total * block_width * block_width)
            clip_factor = jnp.minimum(1.0, clip_limit / jnp.sqrt(sum_squares + 1e-06))
            laid_out, clip_factor = lax.optimization_barrier((laid_out, clip_factor))
        got = lax.all_to_all(laid_out, "fsdp", split_axis=0, concat_axis=0, tiled=True)
        arrived.append(got.reshape(block_width, -1))
    arrived = (arrived[:PARTS], arrived[PARTS:])
    clip = clip_factor.reshape(1, 1)

    updates, fresh = None, []
    slots = (jnp.zeros((1,), jnp.int32), both.astype(jnp.int32).reshape(1))
    for number in range(2):
        start, size = half_starts[number], half_sizes[number]
        update, new_block = precondition(
            slots[number], clip, arrived[number], held_sketches
        )
        fresh.append(new_block)
        returned = lax.all_to_all(
            update.reshape(fsdp_count, row_count, block_width),
            "fsdp",
            split_axis=0,
            concat_axis=0,
            tiled=True,
        )
        targets = my_order[start : start + size]
        owners_here = jnp.sum(
            jnp.where(targets[:, None] == places[None, :], my_owners[None, :], 0), axis=1
        )
        updates = place_blocks(owners_here, targets, returned, per_slice, updates)
    has_first = jnp.sum((mine & (my_half == 0)).astype(jnp.int32)) > 0
    has_second = jnp.sum((mine & (my_half == 1)).astype(jnp.int32)) > 0
    slot_zero = jnp.where(
        has_first, fresh[0], jnp.where(has_second, fresh[1], held_sketches[0])
    )
    slot_one = jnp.where(both, fresh[1], held_sketches[1])
    return (updates, jnp.stack([slot_zero, slot_one])[None, None])


def solution(mesh):
    placed = (P("rep", None, "fsdp", None), P("fsdp", "rep", None, None, None), P())
    return jax.shard_map(
        local,
        mesh=mesh,
        in_specs=placed,
        out_specs=(P("rep", "fsdp", None), P("fsdp", "rep", None, None, None)),
        check_vma=False,
    )
```
